16 devices in a mesh: data: 4 (over z, y), model: 4 (over x, core).
Axes of the slice: x: 2, y: 2, z: 2, core: 2. Of those that a mesh axis runs over, the one named last changes fastest.
Arguments:
- x: bfloat16 [512, 128, 640], P('data'), parts along dimension 0
- w_in: bfloat16 [640, 4, 2048], P(None, None, 'model')
- w_rec: bfloat16 [2048, 4, 2048], P(None, None, 'model')
- gate_bias: float32 [4, 2048], P(None, 'model')
- h_init: float32 [512, 2048], P('data', 'model'), parts along dimension 0
- c_init: float32 [512, 2048], P('data', 'model'), parts along dimension 0
Outputs:
- output 1: bfloat16 [512, 128, 2048], P('data', None, 'model'), parts along dimension 0
- output 2: float32 [512, 2048], P('data', 'model'), parts along dimension 0
- output 3: float32 [512, 2048], P('data', 'model'), parts along dimension 0
There are 4 independent parts. The reference program is written for one: setup_inputs(seed, part) draws one part's arguments, and reference() takes and returns one part's arrays. A program takes and returns all parts, laid end to end along the dimension named above; an argument that names none is the same for every part.
All inputs are finite; a program needn't handle non-finite values.
Results may differ from the reference program's by a relative error of at most 0.00728457.
Values are sent between devices in bfloat16 or wider.
A program may use at most 1 GiB of HBM per device.

```python
import jax
import jax.numpy as jnp
from jax import lax

BATCH_ROWS = 128
TIME_STEPS = 128
INPUT_DIM = 640
HIDDEN_DIM = 2048


def setup_inputs(seed: int = 0, part: int = 0) -> dict:
    part_keys = jax.random.split(jax.random.fold_in(jax.random.key(seed), part), 3)
    shared_keys = jax.random.split(jax.random.key(seed + 1), 3)
    x = jax.random.normal(part_keys[0], (BATCH_ROWS, TIME_STEPS, INPUT_DIM), jnp.float32)
    h_init = jnp.tanh(jax.random.normal(part_keys[1], (BATCH_ROWS, HIDDEN_DIM), jnp.float32))
    c_init = jax.random.normal(part_keys[2], (BATCH_ROWS, HIDDEN_DIM), jnp.float32)
    w_in = jax.random.normal(shared_keys[0], (INPUT_DIM, 4, HIDDEN_DIM), jnp.float32) * (INPUT_DIM ** -0.5)
    w_rec = jax.random.normal(shared_keys[1], (HIDDEN_DIM, 4, HIDDEN_DIM), jnp.float32) * (1.5 * HIDDEN_DIM ** -0.5)
    offsets = jnp.array([0.0, 3.0, 0.0, 0.0], jnp.float32)[:, None]
    gate_bias = 0.5 * jax.random.normal(shared_keys[2], (4, HIDDEN_DIM), jnp.float32) + offsets
    return {
        "x": x.astype(jnp.bfloat16),
        "w_in": w_in.astype(jnp.bfloat16),
        "w_rec": w_rec.astype(jnp.bfloat16),
        "gate_bias": gate_bias,
        "h_init": h_init,
        "c_init": c_init,
    }


def reference(x, w_in, w_rec, gate_bias, h_init, c_init):
    in_dim = w_in.shape[0]
    hidden = w_rec.shape[0]
    batch_rows = x.shape[0]
    w_in_flat = w_in.reshape(in_dim, 4 * hidden)
    w_rec_flat = w_rec.reshape(hidden, 4 * hidden)

    def step_fn(carry_in, x_step):
        h_prev, c_prev = carry_in
        gate_pre = jnp.dot(x_step, w_in_flat, preferred_element_type=jnp.float32) + jnp.dot(
            h_prev.astype(jnp.bfloat16), w_rec_flat, preferred_element_type=jnp.float32)
        gate_pre = gate_pre.reshape(batch_rows, 4, hidden) + gate_bias
        c_next = jax.nn.sigmoid(gate_pre[:, 1]) * c_prev + jax.nn.sigmoid(gate_pre[:, 0]) * jnp.tanh(gate_pre[:, 3])
        h_next = jax.nn.sigmoid(gate_pre[:, 2]) * jnp.tanh(c_next)
        return (h_next, c_next), h_next.astype(jnp.bfloat16)

    (h_last, c_last), y_steps = lax.scan(step_fn, (h_init, c_init), jnp.swapaxes(x, 0, 1))
    return jnp.swapaxes(y_steps, 0, 1), h_last, c_last
```

```python
import functools

import jax
import jax.numpy as jnp
from jax import lax
from jax.experimental import pallas as pl
from jax.experimental.pallas import tpu as pltpu
from jax.sharding import PartitionSpec as P

MESH = pl.DeviceIdType.MESH
F32 = jnp.float32
BF16 = jnp.bfloat16
SLOTS = 4
XSLOTS = 3


def sigmoid(v):
    return 0.5 * jnp.tanh(0.5 * v) + 0.5


def recurrent_kernel(steps, rows, units, tile,
                     xp_ref, own_ref, other_ref, h0_ref, c0_ref,
                     y_ref, hl_ref, cl_ref,
                     w_ref, hbuf, c_ref, hf_ref, acc, xbuf,
                     wsem, xsem, hsend, hrecv, ylocal, ysend, yrecv, fin):
    per = units // tile
    nb = 2 * per
    me = lax.axis_index("model")
    core = me % 2
    chip = me // 2
    sib = 2 * chip + (1 - core)
    twin = 2 * (1 - chip) + core
    sibtwin = 2 * (1 - chip) + (1 - core)
    row0 = pl.multiple_of(chip * rows, rows)

    barrier = pltpu.get_barrier_semaphore()
    for peer in (sib, twin):
        pl.semaphore_signal(barrier, inc=1, device_id={"model": peer}, device_id_type=MESH)

    loads = []
    for half, src in enumerate((own_ref, other_ref)):
        for kb, blk in enumerate((me, twin, sib, sibtwin)):
            loads.append(pltpu.make_async_copy(
                src.at[:, pl.ds(pl.multiple_of(blk * units, units), units), :],
                w_ref.at[half, :, pl.ds(kb * units, units), :],
                wsem.at[half, kb]))
    for cp in loads:
        cp.start()

    def xcopy(t, slot):
        return pltpu.make_async_copy(xp_ref.at[t], xbuf.at[slot], xsem.at[slot])

    def hcopy(slot, j):
        return pltpu.make_async_remote_copy(
            src_ref=hbuf.at[slot, j], dst_ref=hbuf.at[slot, nb + j],
            send_sem=hsend.at[slot, j], recv_sem=hrecv.at[slot, j],
            device_id={"model": sib}, device_id_type=MESH)

    def ydst(t, j):
        return y_ref.at[t, pl.ds(row0, rows), pl.ds((j % per) * tile, tile)]

    def ycopy(t, slot, j):
        if j < per:
            return pltpu.make_async_copy(hbuf.at[slot, j], ydst(t, j), ylocal.at[slot, j])
        return pltpu.make_async_remote_copy(
            src_ref=hbuf.at[slot, j], dst_ref=ydst(t, j),
            send_sem=ysend.at[slot, j - per], recv_sem=yrecv,
            device_id={"model": twin}, device_id_type=MESH)

    def wait_y(slot, j):
        if j < per:
            ycopy(0, slot, j).wait()
        else:
            ycopy(0, slot, j).wait_send()

    for t in range(XSLOTS):
        xcopy(t, t).start()
    c_ref[...] = c0_ref[...]
    for j in range(nb):
        hbuf[0, j] = h0_ref[:, j * tile:(j + 1) * tile]

    pl.semaphore_wait(barrier, 2)
    for j in range(nb):
        hcopy(0, j).start()
    for cp in loads:
        cp.wait()

    def part_own(slot, xslot):
        h = [hbuf[slot, kb] for kb in range(nb)]
        for j in range(nb):
            half, nn = divmod(j, per)
            for k in range(4):
                s = None
                for kb in range(nb):
                    d = jnp.dot(h[kb], w_ref[half, k, kb * tile:(kb + 1) * tile, nn * tile:(nn + 1) * tile],
                                preferred_element_type=F32)
                    s = d if s is None else s + d
                col = (half * 4 + k) * units + nn * tile
                acc[j, k] = s + xbuf[xslot, :, pl.ds(col, tile)]

    def part_rest(t, slot, nslot, last):
        h = [hbuf[slot, nb + kb] for kb in range(nb)]
        for j in range(nb):
            half, nn = divmod(j, per)
            g = []
            for k in range(4):
                s = None
                for kb in range(nb):
                    row = (nb + kb) * tile
                    d = jnp.dot(h[kb], w_ref[half, k, row:row + tile, nn * tile:(nn + 1) * tile],
                                preferred_element_type=F32)
                    s = d if s is None else s + d
                g.append(s + acc[j, k])
            c = sigmoid(g[1]) * c_ref[j] + sigmoid(g[0]) * jnp.tanh(g[3])
            c_ref[j] = c
            hv = sigmoid(g[2]) * jnp.tanh(c)
            hbuf[nslot, j] = hv.astype(BF16)
            if last:
                hf_ref[j] = hv
            else:
                hcopy(nslot, j).start()
            ycopy(t, nslot, j).start()

    xcopy(0, 0).wait()
    part_own(0, 0)

    def step(t, carry):
        slot = lax.rem(t, SLOTS)
        nslot = lax.rem(t + 1, SLOTS)

        @pl.when(t >= SLOTS)
        def _():
            for j in range(nb):
                hcopy(nslot, j).wait_send()
                wait_y(nslot, j)

        @pl.when(jnp.logical_and(t >= SLOTS - 1, t < SLOTS))
        def _():
            for j in range(nb):
                hcopy(nslot, j).wait_send()

        @pl.when(t + XSLOTS < steps)
        def _():
            xcopy(t + XSLOTS, lax.rem(t, XSLOTS)).start()
        xslot = lax.rem(t + 1, XSLOTS)
        xcopy(0, xslot).wait()
        for j in range(nb):
            hcopy(slot, j).wait_recv()
        part_rest(t, slot, nslot, False)
        part_own(nslot, xslot)
        return carry

    lax.fori_loop(0, steps - 1, step, 0)

    t = steps - 1
    slot, nslot = t % SLOTS, (t + 1) % SLOTS
    for j in range(nb):
        hcopy(nslot, j).wait_send()
        wait_y(nslot, j)
        hcopy(slot, j).wait_recv()
    part_rest(t, slot, nslot, True)

    ends = []
    for n, (src, dst) in enumerate(((hf_ref, hl_ref), (c_ref, cl_ref))):
        for j in range(nb):
            d = dst.at[pl.ds(row0, rows), pl.ds((j % per) * tile, tile)]
            if j < per:
                cp = pltpu.make_async_copy(src.at[j], d, fin.at[0, n, j])
            else:
                cp = pltpu.make_async_remote_copy(
                    src_ref=src.at[j], dst_ref=d,
                    send_sem=fin.at[0, n, j], recv_sem=fin.at[1, n, j],
                    device_id={"model": twin}, device_id_type=MESH)
            cp.start()
            ends.append(cp)
    for s in range(1, SLOTS):
        q = (nslot + s) % SLOTS
        for j in range(nb):
            hcopy(q, j).wait_send()
            wait_y(q, j)
    for j in range(nb):
        wait_y(nslot, j)
    theirs = y_ref.at[:, pl.ds(pl.multiple_of((1 - chip) * rows, rows), rows), :]
    pltpu.make_async_copy(theirs, theirs, yrecv).wait()
    for cp in ends:
        cp.wait()


def recurrent(xp, own, other, h0, c0, batch, tile=256):
    steps, rows, _ = xp.shape
    units = own.shape[2]
    hidden = own.shape[1]
    nb = 2 * (units // tile)
    any_spec = pl.BlockSpec(memory_space=pl.ANY)
    vmem = pl.BlockSpec(memory_space=pltpu.VMEM)
    return pl.pallas_call(
        functools.partial(recurrent_kernel, steps, rows, units, tile),
        out_shape=(jax.ShapeDtypeStruct((steps, batch, units), BF16),
                   jax.ShapeDtypeStruct((batch, units), F32),
                   jax.ShapeDtypeStruct((batch, units), F32)),
        in_specs=[any_spec, any_spec, any_spec, vmem, vmem],
        out_specs=(any_spec, any_spec, any_spec),
        scratch_shapes=[
            pltpu.VMEM((2, 4, hidden, units), BF16),
            pltpu.VMEM((SLOTS, 2 * nb, rows, tile), BF16),
            pltpu.VMEM((nb, rows, tile), F32),
            pltpu.VMEM((nb, rows, tile), F32),
            pltpu.VMEM((nb, 4, rows, tile), F32),
            pltpu.VMEM((XSLOTS, rows, 8 * units), F32),
            pltpu.SemaphoreType.DMA((2, 4)),
            pltpu.SemaphoreType.DMA((XSLOTS,)),
            pltpu.SemaphoreType.DMA((SLOTS, nb)),
            pltpu.SemaphoreType.DMA((SLOTS, nb)),
            pltpu.SemaphoreType.DMA((SLOTS, nb // 2)),
            pltpu.SemaphoreType.DMA((SLOTS, nb // 2)),
            pltpu.SemaphoreType.DMA,
            pltpu.SemaphoreType.DMA((2, 2, nb)),
        ],
        compiler_params=pltpu.CompilerParams(
            collective_id=0, has_side_effects=True, vmem_limit_bytes=60 * 1024 * 1024),
        name="recurrent",
    )(xp, own, other, h0, c0)


def solution(mesh):
    n_model = mesh.shape["model"]
    swap = [(i, (i + n_model // 2) % n_model) for i in range(n_model)]

    def local_fn(x, w_in, w_rec, gate_bias, h_init, c_init):
        in_dim = w_in.shape[0]
        hidden, _, units = w_rec.shape
        batch, steps, _ = x.shape
        rows = batch // 2
        tile = 256
        nb = 2 * (units // tile)
        data = lax.axis_index("data")
        chip = lax.axis_index("model") // 2
        row0 = chip * rows
        orow0 = (1 - chip) * rows

        w4 = jnp.concatenate([w_rec.swapaxes(0, 1), w_in.swapaxes(0, 1)], axis=1)
        quarter = lax.dynamic_index_in_dim(w4, data, 0, keepdims=False)
        o4 = lax.all_gather(lax.ppermute(quarter, "model", swap), "data", axis=0)

        small = jnp.concatenate([
            lax.dynamic_slice_in_dim(c_init, orow0, rows, 0),
            lax.dynamic_slice_in_dim(h_init, orow0, rows, 0),
            gate_bias], axis=0)
        small_o = lax.ppermute(small, "model", swap)
        c_own = lax.dynamic_slice_in_dim(c_init, row0, rows, 0)
        h_own = lax.dynamic_slice_in_dim(h_init, row0, rows, 0)
        c0 = jnp.concatenate([c_own, small_o[:rows]], axis=1).reshape(rows, nb, tile).swapaxes(0, 1)
        h0 = jnp.concatenate([h_own, small_o[rows:2 * rows]], axis=1).astype(BF16)
        bias = jnp.concatenate([gate_bias.reshape(-1), small_o[2 * rows:].reshape(-1)])

        wx = jnp.concatenate([w4[:, hidden:], o4[:, hidden:]], axis=0)
        xt = lax.dynamic_slice_in_dim(x, row0, rows, 0).swapaxes(0, 1)
        xp = jnp.einsum("trd,gdu->trgu", xt, wx, preferred_element_type=F32)
        xp = xp.reshape(steps, rows, 8 * units) + bias

        y, h_last, c_last = recurrent(xp, w4[:, :hidden], o4[:, :hidden], h0, c0, batch, tile)
        return y.swapaxes(0, 1), h_last, c_last

    return jax.shard_map(
        local_fn,
        mesh=mesh,
        in_specs=(P("data", None, None), P(None, None, "model"), P(None, None, "model"),
                  P(None, "model"), P("data", "model"), P("data", "model")),
        out_specs=(P("data", None, "model"), P("data", "model"), P("data", "model")),
        check_vma=False,
    )
```

```python
import jax
import jax.numpy as jnp
from jax import lax
from jax.experimental import pallas as pl
from jax.experimental.pallas import tpu as pltpu
from jax.sharding import PartitionSpec as P

MESH = pl.DeviceIdType.MESH
F32 = jnp.float32
BF16 = jnp.bfloat16
SLOTS = 4
XSLOTS = 3
TC = 8
CH = 128


def sigmoid(v):
    return 0.5 * jnp.tanh(0.5 * v) + 0.5


def lstm_kernel(steps, rows, units, tile, in_dim,
                xt_ref, wx_ref, wh_ref, bias_ref, h0_ref, c0_ref,
                y_ref, hl_ref, cl_ref, xp_ref,
                w_ref, hbuf, c_ref, hf_ref, acc, xbuf, bias_v, xin, xout,
                wsem, isem, rsem, ssem, insem, outsem,
                xsem, hsend, hrecv, ylocal, ysend, yrecv, fin):
    per = units // tile
    nb = 2 * per
    me = lax.axis_index("model")
    data = lax.axis_index("data")
    core = me % 2
    chip = me // 2
    sib = 2 * chip + (1 - core)
    twin = 2 * (1 - chip) + core
    sibtwin = 2 * (1 - chip) + (1 - core)
    ynbr = 2 * (data // 2) + (1 - data % 2)
    znbr = 2 * (1 - data // 2) + data % 2
    diag = 2 * (1 - data // 2) + (1 - data % 2)
    row0 = pl.multiple_of(chip * rows, rows)
    orow0 = pl.multiple_of((1 - chip) * rows, rows)

    hbuf[...] = jnp.zeros(hbuf.shape, BF16)
    barrier = pltpu.get_barrier_semaphore()
    for peer in ({"model": sib}, {"model": twin}, {"data": ynbr}, {"data": znbr}):
        pl.semaphore_signal(barrier, inc=1, device_id=peer, device_id_type=MESH)

    loads = [pltpu.make_async_copy(wx_ref, w_ref.at[0, :, pl.ds(0, in_dim), :], wsem.at[0])]
    for kb, blk in enumerate((me, twin, sib, sibtwin)):
        loads.append(pltpu.make_async_copy(
            wh_ref.at[:, pl.ds(pl.multiple_of(blk * units, units), units), :],
            w_ref.at[0, :, pl.ds(in_dim + kb * units, units), :],
            wsem.at[1 + kb]))
    for cp in loads:
        cp.start()

    def xin_copy(c, slot):
        return pltpu.make_async_copy(
            xt_ref.at[pl.ds(c * TC, TC)], xin.at[slot], insem.at[slot])

    xin_copy(0, 0).start()
    own_init = [pltpu.make_async_copy(bias_ref, bias_v.at[0], isem.at[0, 0])]
    for n in range(per):
        cols = pl.ds(n * tile, tile)
        own_init.append(pltpu.make_async_copy(h0_ref.at[pl.ds(row0, rows), cols], hf_ref.at[n], isem.at[0, 1 + n]))
        own_init.append(pltpu.make_async_copy(c0_ref.at[pl.ds(row0, rows), cols], c_ref.at[n], isem.at[0, 1 + per + n]))
    for cp in own_init:
        cp.start()

    pl.semaphore_wait(barrier, 4)

    n_chunks = (in_dim + 4 * units) // CH

    def landing(g, s):
        return w_ref.at[1, g, pl.ds(pl.multiple_of(s * CH, CH), CH), :]

    def from_twin(rel, g, s):
        if s * CH < in_dim:
            src = wx_ref.at[g, pl.ds(s * CH, CH), :]
        else:
            kb, off = divmod(s * CH - in_dim, units)
            blk = (twin, me, sibtwin, sib)[kb]
            src = wh_ref.at[g, pl.ds(pl.multiple_of(blk * units + off, CH), CH), :]
        return pltpu.make_async_remote_copy(
            src_ref=src, dst_ref=landing(g, s),
            send_sem=ssem.at[0 if rel == 0 else 1, s], recv_sem=rsem.at[rel, s],
            device_id={"model": twin}, device_id_type=MESH)

    def relay(peer, link, rel, g, s):
        return pltpu.make_async_remote_copy(
            src_ref=landing(g, s), dst_ref=landing(g, s),
            send_sem=ssem.at[link, s], recv_sem=rsem.at[rel, s],
            device_id={"data": peer}, device_id_type=MESH)

    other_init = [pltpu.make_async_remote_copy(
        src_ref=bias_ref, dst_ref=bias_v.at[1], send_sem=isem.at[1, 0], recv_sem=isem.at[2, 0],
        device_id={"model": twin}, device_id_type=MESH)]
    for n in range(per):
        cols = pl.ds(n * tile, tile)
        for src, dst, at in ((h0_ref, hf_ref, 1), (c0_ref, c_ref, 1 + per)):
            other_init.append(pltpu.make_async_remote_copy(
                src_ref=src.at[pl.ds(orow0, rows), cols], dst_ref=dst.at[per + n],
                send_sem=isem.at[1, at + n], recv_sem=isem.at[2, at + n],
                device_id={"model": twin}, device_id_type=MESH))
    for s in range(n_chunks):
        from_twin(0, data, s).start()
        if s % 3 == 0:
            from_twin(3, diag, s).start()
        if s == 4:
            for cp in other_init:
                cp.start()

    def forward(s):
        relay(ynbr, 2, 0, data, s).wait_recv()
        relay(ynbr, 2, 1, data, s).start()
        relay(znbr, 3, 2, data, s).start()

    def forward_diag(s):
        relay(ynbr, 2, 1, data, s).wait_recv()
        relay(znbr, 3, 2, data, s).wait_recv()

        @pl.when(lax.rem(s, 3) == 1)
        def _():
            relay(ynbr, 4, 3, znbr, s).start()

        @pl.when(lax.rem(s, 3) == 2)
        def _():
            relay(znbr, 5, 3, ynbr, s).start()

    def xout_copy(half, c, slot):
        return pltpu.make_async_copy(
            xout.at[slot], xp_ref.at[pl.ds(c * TC, TC), pl.ds(half * 4 * per, 4 * per)], outsem.at[slot])

    def project(it, carry):
        half = it // (steps // TC)
        c = lax.rem(it, steps // TC)
        slot = lax.rem(it, 2)

        @pl.when(slot == 0)
        def _():
            s = it // 2
            forward(s)

            @pl.when(s >= 1)
            def _():
                forward_diag(s - 1)

        @pl.when(it == steps // TC)
        def _():
            for s in range(in_dim // CH):
                relay(ynbr, 4, 3, diag, s).wait_recv()
            other_init[0].wait_recv()

        xin_copy(c, slot).wait()

        @pl.when(it + 1 < 2 * (steps // TC))
        def _():
            xin_copy(lax.rem(it + 1, steps // TC), 1 - slot).start()

        @pl.when(it >= 2)
        def _():
            xout_copy(half, c, slot).wait()

        xv = xin[slot].reshape(TC * rows, in_dim)
        for k in range(4):
            for nn in range(per):
                cols = slice(nn * tile, (nn + 1) * tile)
                g = jnp.dot(xv, w_ref[half, k, 0:in_dim, cols], preferred_element_type=F32)
                xout[slot, :, k * per + nn] = (g + bias_v[half, k:k + 1, cols]).reshape(TC, rows, tile)
        xout_copy(half, c, slot).start()
        return carry

    for cp in own_init + loads:
        cp.wait()
    n_proj = 2 * (steps // TC)
    lax.fori_loop(0, n_proj, project, 0)
    for slot in range(2):
        xout_copy(0, 0, slot).wait()

    def xcopy(t, slot):
        return pltpu.make_async_copy(xp_ref.at[t], xbuf.at[slot], xsem.at[slot])

    for t in range(XSLOTS):
        xcopy(t, t).start()

    def tail(s, carry):
        forward(s)
        forward_diag(s - 1)
        return carry

    lax.fori_loop(n_proj // 2, n_chunks, tail, 0)
    forward_diag(n_chunks - 1)

    def hcopy(slot):
        return pltpu.make_async_remote_copy(
            src_ref=hbuf.at[slot, 0, pl.ds(0, rows)], dst_ref=hbuf.at[slot, 1, pl.ds(0, rows)],
            send_sem=hsend.at[slot], recv_sem=hrecv.at[slot],
            device_id={"model": sib}, device_id_type=MESH)

    def ylocal_copy(t, slot):
        return pltpu.make_async_copy(
            hbuf.at[slot, 0, pl.ds(0, rows), pl.ds(0, units)], y_ref.at[t, pl.ds(row0, rows)], ylocal.at[slot])

    def ytwin_copy(t, slot):
        return pltpu.make_async_remote_copy(
            src_ref=hbuf.at[slot, 0, pl.ds(0, rows), pl.ds(units, units)], dst_ref=y_ref.at[t, pl.ds(row0, rows)],
            send_sem=ysend.at[slot], recv_sem=yrecv,
            device_id={"model": twin}, device_id_type=MESH)

    def wait_y(slot):
        ylocal_copy(0, slot).wait()
        ytwin_copy(0, slot).wait_send()

    for cp in other_init[1:]:
        cp.wait_recv()
    for j in range(nb):
        hbuf[0, 0, 0:rows, j * tile:(j + 1) * tile] = hf_ref[j].astype(BF16)
    hcopy(0).start()
    for s in range(in_dim // CH, n_chunks):
        relay(ynbr, 4, 3, diag, s).wait_recv()

    deep = nb * tile
    cut = deep // 2

    def product(slot, side, j, k, lo, hi):
        half, nn = divmod(j, per)
        row = in_dim + side * deep
        w = w_ref[half, k, row + lo:row + hi, nn * tile:(nn + 1) * tile]
        return jnp.dot(hbuf[slot, side, :, lo:hi], w, preferred_element_type=F32)[:rows]

    def part_own(slot, xslot, stage):
        for j in range(nb):
            half, nn = divmod(j, per)
            for k in range(4):
                if j < nb // 2:
                    if stage == 0:
                        acc[j, k] = product(slot, 0, j, k, 0, cut) + xbuf[xslot, (half * 4 + k) * per + nn]
                    else:
                        acc[j, k] = product(slot, 0, j, k, cut, deep) + acc[j, k]
                elif stage == 1:
                    acc[j, k] = product(slot, 0, j, k, 0, deep) + xbuf[xslot, (half * 4 + k) * per + nn]

    def part_rest(slot, nslot, last):
        for j in range(nb):
            g = [product(slot, 1, j, k, 0, deep) + acc[j, k] for k in range(4)]
            c = sigmoid(g[1]) * c_ref[j] + sigmoid(g[0]) * jnp.tanh(g[3])
            c_ref[j] = c
            hv = sigmoid(g[2]) * jnp.tanh(c)
            hbuf[nslot, 0, 0:rows, j * tile:(j + 1) * tile] = hv.astype(BF16)
            if last:
                hf_ref[j] = hv

    xcopy(0, 0).wait()
    part_own(0, 0, 0)
    part_own(0, 0, 1)

    def step(t, carry):
        slot = lax.rem(t, SLOTS)
        nslot = lax.rem(t + 1, SLOTS)

        @pl.when(t >= SLOTS)
        def _():
            hcopy(nslot).wait_send()
            wait_y(nslot)

        @pl.when(t == SLOTS - 1)
        def _():
            hcopy(nslot).wait_send()

        @pl.when(t + XSLOTS < steps)
        def _():
            xcopy(t + XSLOTS, lax.rem(t, XSLOTS)).start()
        xslot = lax.rem(t + 1, XSLOTS)
        xcopy(0, xslot).wait()
        hcopy(slot).wait_recv()
        part_rest(slot, nslot, False)
        part_own(nslot, xslot, 0)
        hcopy(nslot).start()
        ylocal_copy(t, nslot).start()
        ytwin_copy(t, nslot).start()
        part_own(nslot, xslot, 1)
        return carry

    lax.fori_loop(0, steps - 1, step, 0)

    t = steps - 1
    slot, nslot = t % SLOTS, (t + 1) % SLOTS
    hcopy(nslot).wait_send()
    wait_y(nslot)
    hcopy(slot).wait_recv()
    part_rest(slot, nslot, True)
    ylocal_copy(t, nslot).start()
    ytwin_copy(t, nslot).start()

    ends = []
    for n, (src, dst) in enumerate(((hf_ref, hl_ref), (c_ref, cl_ref))):
        for j in range(nb):
            d = dst.at[pl.ds(row0, rows), pl.ds((j % per) * tile, tile)]
            if j < per:
                cp = pltpu.make_async_copy(src.at[j], d, fin.at[0, n, j])
            else:
                cp = pltpu.make_async_remote_copy(
                    src_ref=src.at[j], dst_ref=d,
                    send_sem=fin.at[0, n, j], recv_sem=fin.at[1, n, j],
                    device_id={"model": twin}, device_id_type=MESH)
            cp.start()
            ends.append(cp)
    for s in range(1, SLOTS):
        q = (nslot + s) % SLOTS
        hcopy(q).wait_send()
        wait_y(q)
    wait_y(nslot)
    theirs = y_ref.at[:, pl.ds(pl.multiple_of((1 - chip) * rows, rows), rows), :]
    pltpu.make_async_copy(theirs, theirs, yrecv).wait()
    for cp in ends:
        cp.wait()
    for cp in other_init:
        cp.wait_send()
    for s in range(n_chunks):
        from_twin(0, data, s).wait_send()
        relay(ynbr, 2, 1, data, s).wait_send()
        relay(znbr, 3, 2, data, s).wait_send()
        if s % 3 == 0:
            from_twin(3, diag, s).wait_send()
        else:
            relay(ynbr, 3 + s % 3, 3, diag, s).wait_send()


def lstm(xt, wx, wh, bias, h0, c0, tile=256):
    steps, rows, in_dim = xt.shape
    hidden, units = wh.shape[1:]
    batch = h0.shape[0]
    nb = 2 * (units // tile)
    n_chunks = (in_dim + hidden) // CH
    any_spec = pl.BlockSpec(memory_space=pl.ANY)

    def kernel(*refs):
        lstm_kernel(steps, rows, units, tile, in_dim, *refs)

    return pl.pallas_call(
        kernel,
        out_shape=(jax.ShapeDtypeStruct((steps, batch, units), BF16),
                   jax.ShapeDtypeStruct((batch, units), F32),
                   jax.ShapeDtypeStruct((batch, units), F32),
                   jax.ShapeDtypeStruct((steps, 4 * nb, rows, tile), F32)),
        in_specs=[any_spec] * 6,
        out_specs=(any_spec,) * 4,
        scratch_shapes=[
            pltpu.VMEM((2, 4, in_dim + hidden, units), BF16),
            pltpu.VMEM((SLOTS, 2, 2 * rows, nb * tile), BF16),
            pltpu.VMEM((nb, rows, tile), F32),
            pltpu.VMEM((nb, rows, tile), F32),
            pltpu.VMEM((nb, 4, rows, tile), F32),
            pltpu.VMEM((XSLOTS, 4 * nb, rows, tile), F32),
            pltpu.VMEM((2, 8, units), F32),
            pltpu.VMEM((2, TC, rows, in_dim), BF16),
            pltpu.VMEM((2, TC, 2 * nb, rows, tile), F32),
            pltpu.SemaphoreType.DMA((5,)),
            pltpu.SemaphoreType.DMA((3, 1 + nb)),
            pltpu.SemaphoreType.DMA((4, n_chunks)),
            pltpu.SemaphoreType.DMA((6, n_chunks)),
            pltpu.SemaphoreType.DMA((2,)),
            pltpu.SemaphoreType.DMA((2,)),
            pltpu.SemaphoreType.DMA((XSLOTS,)),
            pltpu.SemaphoreType.DMA((SLOTS,)),
            pltpu.SemaphoreType.DMA((SLOTS,)),
            pltpu.SemaphoreType.DMA((SLOTS,)),
            pltpu.SemaphoreType.DMA((SLOTS,)),
            pltpu.SemaphoreType.DMA,
            pltpu.SemaphoreType.DMA((2, 2, nb)),
        ],
        compiler_params=pltpu.CompilerParams(
            collective_id=0, has_side_effects=True, vmem_limit_bytes=60 * 1024 * 1024),
        name="recurrent",
    )(xt, wx, wh, bias, h0, c0)


def solution(mesh):
    def local_fn(x, w_in, w_rec, gate_bias, h_init, c_init):
        rows = x.shape[0] // 2
        row0 = (lax.axis_index("model") // 2) * rows
        xt = lax.dynamic_slice_in_dim(x, row0, rows, 0).swapaxes(0, 1)
        bias = jnp.pad(gate_bias, ((0, 4), (0, 0)))
        y, h_last, c_last, _ = lstm(xt, w_in.swapaxes(0, 1), w_rec.swapaxes(0, 1), bias, h_init, c_init)
        return y.swapaxes(0, 1), h_last, c_last

    return jax.shard_map(
        local_fn,
        mesh=mesh,
        in_specs=(P("data", None, None), P(None, None, "model"), P(None, None, "model"),
                  P(None, "model"), P("data", "model"), P("data", "model")),
        out_specs=(P("data", None, "model"), P("data", "model"), P("data", "model")),
        check_vma=False,
    )
```

```python
import jax
import jax.numpy as jnp
from jax import lax
from jax.experimental import pallas as pl
from jax.experimental.pallas import tpu as pltpu
from jax.sharding import PartitionSpec as P

MESH = pl.DeviceIdType.MESH
F32 = jnp.float32
BF16 = jnp.bfloat16
SLOTS = 4
XSLOTS = 3
TX = 16
TC = 8
LAG = 2
DELAY = 2
AHEAD = 5
CH = 128


def sigmoid(v):
    return 0.5 * jnp.tanh(0.5 * v) + 0.5


def lstm_kernel(steps, rows, units, tile, in_dim,
                x_ref, wx_ref, wh_ref, bias_ref, h0_ref, c0_ref,
                y_ref, hl_ref, cl_ref, xp_ref,
                w_ref, hbuf, c_ref, hf_ref, acc, xbuf, bias_v, xraw, xf, xt, xout,
                wsem, isem, rsem, ssem, insem, outsem,
                xsem, hsend, hrecv, ylocal, ysend, yrecv, fin):
    per = units // tile
    nb = 2 * per
    me = lax.axis_index("model")
    data = lax.axis_index("data")
    core = me % 2
    chip = me // 2
    sib = 2 * chip + (1 - core)
    twin = 2 * (1 - chip) + core
    sibtwin = 2 * (1 - chip) + (1 - core)
    ynbr = 2 * (data // 2) + (1 - data % 2)
    znbr = 2 * (1 - data // 2) + data % 2
    diag = 2 * (1 - data // 2) + (1 - data % 2)
    row0 = pl.multiple_of(chip * rows, rows)
    orow0 = pl.multiple_of((1 - chip) * rows, rows)

    hbuf[...] = jnp.zeros(hbuf.shape, BF16)
    barrier = pltpu.get_barrier_semaphore()
    for peer in ({"model": sib}, {"model": twin}, {"data": ynbr}, {"data": znbr}):
        pl.semaphore_signal(barrier, inc=1, device_id=peer, device_id_type=MESH)

    loads = [pltpu.make_async_copy(wx_ref, w_ref.at[0, :, pl.ds(0, in_dim), :], wsem.at[0])]
    for kb, blk in enumerate((me, twin, sib, sibtwin)):
        loads.append(pltpu.make_async_copy(
            wh_ref.at[:, pl.ds(pl.multiple_of(blk * units, units), units), :],
            w_ref.at[0, :, pl.ds(in_dim + kb * units, units), :],
            wsem.at[1 + kb]))
    for cp in loads:
        cp.start()

    def x_copy(n, slot):
        return pltpu.make_async_copy(
            x_ref.at[pl.ds(row0, rows), pl.ds(pl.multiple_of(n * TX, TX), TX)], xraw.at[slot], insem.at[slot])

    x_copy(0, 0).start()

    own_init = [pltpu.make_async_copy(bias_ref, bias_v.at[0], isem.at[0, 0])]
    for n in range(per):
        cols = pl.ds(n * tile, tile)
        own_init.append(pltpu.make_async_copy(h0_ref.at[pl.ds(row0, rows), cols], hf_ref.at[n], isem.at[0, 1 + n]))
        own_init.append(pltpu.make_async_copy(c0_ref.at[pl.ds(row0, rows), cols], c_ref.at[n], isem.at[0, 1 + per + n]))
    for cp in own_init:
        cp.start()

    pl.semaphore_wait(barrier, 4)

    n_chunks = (in_dim + 4 * units) // CH

    def landing(g, s):
        return w_ref.at[1, g, pl.ds(pl.multiple_of(s * CH, CH), CH), :]

    wx_chunks = in_dim // CH

    def from_twin(rel, g, s, of_wx):
        if of_wx:
            src = wx_ref.at[g, pl.ds(pl.multiple_of(s * CH, CH), CH), :]
        else:
            kb = (s - wx_chunks) * CH // units
            off = (s - wx_chunks) * CH % units
            blk = 2 * ((chip + 1 + kb) % 2) + (core + kb // 2) % 2
            src = wh_ref.at[g, pl.ds(pl.multiple_of(blk * units + off, CH), CH), :]
        return pltpu.make_async_remote_copy(
            src_ref=src, dst_ref=landing(g, s),
            send_sem=ssem.at[0 if rel == 0 else 1, s], recv_sem=rsem.at[rel, s],
            device_id={"model": twin}, device_id_type=MESH)

    def relay(peer, link, rel, g, s):
        return pltpu.make_async_remote_copy(
            src_ref=landing(g, s), dst_ref=landing(g, s),
            send_sem=ssem.at[link, s], recv_sem=rsem.at[rel, s],
            device_id={"data": peer}, device_id_type=MESH)

    other_init = [pltpu.make_async_remote_copy(
        src_ref=bias_ref, dst_ref=bias_v.at[1], send_sem=isem.at[1, 0], recv_sem=isem.at[2, 0],
        device_id={"model": twin}, device_id_type=MESH)]
    for n in range(per):
        cols = pl.ds(n * tile, tile)
        for src, dst, at in ((h0_ref, hf_ref, 1), (c0_ref, c_ref, 1 + per)):
            other_init.append(pltpu.make_async_remote_copy(
                src_ref=src.at[pl.ds(orow0, rows), cols], dst_ref=dst.at[per + n],
                send_sem=isem.at[1, at + n], recv_sem=isem.at[2, at + n],
                device_id={"model": twin}, device_id_type=MESH))
    for s in range(AHEAD):
        from_twin(0, data, s, True).start()
        if s % 3 == 0:
            from_twin(3, diag, s, True).start()
    for cp in other_init:
        cp.start()
    first_late = -(-wx_chunks // 3) * 3
    n_late = len(range(first_late, n_chunks, 3))

    def forward(s):
        relay(ynbr, 2, 0, data, s).wait_recv()
        relay(ynbr, 2, 1, data, s).start()
        relay(znbr, 3, 2, data, s).start()
        nxt = s + AHEAD

        @pl.when(nxt < wx_chunks)
        def _():
            from_twin(0, data, nxt, True).start()

            @pl.when(lax.rem(nxt, 3) == 0)
            def _():
                from_twin(3, diag, nxt, True).start()

        @pl.when(jnp.logical_and(nxt >= wx_chunks, nxt < n_chunks))
        def _():
            from_twin(0, data, nxt, False).start()

        @pl.when(s >= n_chunks - n_late)
        def _():
            from_twin(3, diag, first_late + 3 * (s - (n_chunks - n_late)), False).start()

    def forward_diag(s):
        relay(ynbr, 2, 1, data, s).wait_recv()
        relay(znbr, 3, 2, data, s).wait_recv()

        @pl.when(lax.rem(s, 3) == 1)
        def _():
            relay(ynbr, 4, 3, znbr, s).start()

        @pl.when(lax.rem(s, 3) == 2)
        def _():
            relay(znbr, 5, 3, ynbr, s).start()

    def stage(i):
        @pl.when(i < n_chunks)
        def _():
            forward(i)

        @pl.when(jnp.logical_and(i >= LAG, i < n_chunks + LAG))
        def _():
            forward_diag(i - LAG)

    def xout_copy(half, c, slot):
        return pltpu.make_async_copy(
            xout.at[slot], xp_ref.at[pl.ds(c * TC, TC), pl.ds(half * 4 * per, 4 * per)], outsem.at[slot])

    def project(it, carry):
        half = it // (steps // TC)
        c = lax.rem(it, steps // TC)
        slot = lax.rem(it, 2)

        late = it - steps // TC

        @pl.when(jnp.logical_and(it >= DELAY, late < 0))
        def _():
            stage(it - DELAY)

        @pl.when(jnp.logical_and(late >= 0, lax.rem(late, 3) < 2))
        def _():
            stage(steps // TC - DELAY + late // 3 * 2 + lax.rem(late, 3))

        @pl.when(it == steps // TC)
        def _():
            for s in range(in_dim // CH):
                relay(ynbr, 4, 3, diag, s).wait_recv()
            other_init[0].wait_recv()

        @pl.when(jnp.logical_and(slot == 0, half == 0))
        def _():
            n = it // 2
            xslot = lax.rem(n, 2)
            x_copy(n, xslot).wait()

            @pl.when(n + 1 < steps // TX)
            def _():
                x_copy(n + 1, 1 - xslot).start()

            for f in range(in_dim // 128):
                lanes = slice(f * 128, (f + 1) * 128)
                xf[f] = xraw[xslot, :, :, lanes].astype(F32).reshape(rows * TX, 128)
            for f in range(in_dim // 128):
                lanes = slice(f * 128, (f + 1) * 128)
                for tt in range(TX):
                    xt[n * TX + tt, :, lanes] = xf[f, pl.ds(tt, rows, stride=TX), :].astype(BF16)

        @pl.when(it >= 2)
        def _():
            xout_copy(half, c, slot).wait()

        xv = xt[pl.ds(c * TC, TC)].reshape(TC * rows, in_dim)
        for k in range(4):
            for nn in range(per):
                cols = slice(nn * tile, (nn + 1) * tile)
                g = jnp.dot(xv, w_ref[half, k, 0:in_dim, cols], preferred_element_type=F32)
                xout[slot, :, k * per + nn] = (g + bias_v[half, k:k + 1, cols]).reshape(TC, rows, tile)
        xout_copy(half, c, slot).start()
        return carry

    for cp in own_init + loads:
        cp.wait()
    n_proj = 2 * (steps // TC)
    lax.fori_loop(0, n_proj, project, 0)
    for slot in range(2):
        xout_copy(0, 0, slot).wait()

    def xcopy(t, slot):
        return pltpu.make_async_copy(xp_ref.at[t], xbuf.at[slot], xsem.at[slot])

    for t in range(XSLOTS):
        xcopy(t, t).start()

    def tail(i, carry):
        stage(i)
        return carry

    n_stages = steps // TC - DELAY + sum(i % 3 < 2 for i in range(steps // TC))
    lax.fori_loop(n_stages, max(n_stages, n_chunks + LAG), tail, 0)

    def hcopy(slot):
        return pltpu.make_async_remote_copy(
            src_ref=hbuf.at[slot, 0, pl.ds(0, rows)], dst_ref=hbuf.at[slot, 1, pl.ds(0, rows)],
            send_sem=hsend.at[slot], recv_sem=hrecv.at[slot],
            device_id={"model": sib}, device_id_type=MESH)

    def ylocal_copy(t, slot):
        return pltpu.make_async_copy(
            hbuf.at[slot, 0, pl.ds(0, rows), pl.ds(0, units)], y_ref.at[t, pl.ds(row0, rows)], ylocal.at[slot])

    def ytwin_copy(t, slot):
        return pltpu.make_async_remote_copy(
            src_ref=hbuf.at[slot, 0, pl.ds(0, rows), pl.ds(units, units)], dst_ref=y_ref.at[t, pl.ds(row0, rows)],
            send_sem=ysend.at[slot], recv_sem=yrecv,
            device_id={"model": twin}, device_id_type=MESH)

    def wait_y(slot):
        ylocal_copy(0, slot).wait()
        ytwin_copy(0, slot).wait_send()

    for cp in other_init[1:]:
        cp.wait_recv()
    for j in range(nb):
        hbuf[0, 0, 0:rows, j * tile:(j + 1) * tile] = hf_ref[j].astype(BF16)
    hcopy(0).start()
    deep = nb * tile
    cut = deep // 2

    def product(slot, side, j, k, lo, hi):
        half, nn = divmod(j, per)
        row = in_dim + side * deep
        w = w_ref[half, k, row + lo:row + hi, nn * tile:(nn + 1) * tile]
        return jnp.dot(hbuf[slot, side, :, lo:hi], w, preferred_element_type=F32)[:rows]

    def part_own(slot, xslot, stage):
        for j in range(nb):
            half, nn = divmod(j, per)
            for k in range(4):
                if j < nb // 2:
                    if stage == 0:
                        acc[j, k] = product(slot, 0, j, k, 0, cut) + xbuf[xslot, (half * 4 + k) * per + nn]
                    else:
                        acc[j, k] = product(slot, 0, j, k, cut, deep) + acc[j, k]
                elif stage == 1:
                    acc[j, k] = product(slot, 0, j, k, 0, deep) + xbuf[xslot, (half * 4 + k) * per + nn]

    def part_rest(slot, nslot, last):
        for j in range(nb):
            g = [product(slot, 1, j, k, 0, deep) + acc[j, k] for k in range(4)]
            c = sigmoid(g[1]) * c_ref[j] + sigmoid(g[0]) * jnp.tanh(g[3])
            c_ref[j] = c
            hv = sigmoid(g[2]) * jnp.tanh(c)
            hbuf[nslot, 0, 0:rows, j * tile:(j + 1) * tile] = hv.astype(BF16)
            if last:
                hf_ref[j] = hv

    own_chunks = (in_dim + deep) // CH
    for s in range(in_dim // CH, own_chunks):
        relay(ynbr, 4, 3, diag, s).wait_recv()
    xcopy(0, 0).wait()
    part_own(0, 0, 0)
    part_own(0, 0, 1)
    for s in range(own_chunks, n_chunks):
        relay(ynbr, 4, 3, diag, s).wait_recv()

    def step(t, carry):
        slot = lax.rem(t, SLOTS)
        nslot = lax.rem(t + 1, SLOTS)

        @pl.when(t >= SLOTS)
        def _():
            hcopy(nslot).wait_send()
            wait_y(nslot)

        @pl.when(t == SLOTS - 1)
        def _():
            hcopy(nslot).wait_send()

        @pl.when(t + XSLOTS < steps)
        def _():
            xcopy(t + XSLOTS, lax.rem(t, XSLOTS)).start()
        xslot = lax.rem(t + 1, XSLOTS)
        xcopy(0, xslot).wait()
        hcopy(slot).wait_recv()
        part_rest(slot, nslot, False)
        part_own(nslot, xslot, 0)
        hcopy(nslot).start()
        ylocal_copy(t, nslot).start()
        ytwin_copy(t, nslot).start()
        part_own(nslot, xslot, 1)
        return carry

    lax.fori_loop(0, steps - 1, step, 0)

    t = steps - 1
    slot, nslot = t % SLOTS, (t + 1) % SLOTS
    hcopy(nslot).wait_send()
    wait_y(nslot)
    hcopy(slot).wait_recv()
    part_rest(slot, nslot, True)
    ylocal_copy(t, nslot).start()
    ytwin_copy(t, nslot).start()

    ends = []
    for n, (src, dst) in enumerate(((hf_ref, hl_ref), (c_ref, cl_ref))):
        for j in range(nb):
            d = dst.at[pl.ds(row0, rows), pl.ds((j % per) * tile, tile)]
            if j < per:
                cp = pltpu.make_async_copy(src.at[j], d, fin.at[0, n, j])
            else:
                cp = pltpu.make_async_remote_copy(
                    src_ref=src.at[j], dst_ref=d,
                    send_sem=fin.at[0, n, j], recv_sem=fin.at[1, n, j],
                    device_id={"model": twin}, device_id_type=MESH)
            cp.start()
            ends.append(cp)
    for s in range(1, SLOTS):
        q = (nslot + s) % SLOTS
        hcopy(q).wait_send()
        wait_y(q)
    wait_y(nslot)
    theirs = y_ref.at[:, pl.ds(pl.multiple_of((1 - chip) * rows, rows), rows), :]
    pltpu.make_async_copy(theirs, theirs, yrecv).wait()
    for cp in ends:
        cp.wait()
    for cp in other_init:
        cp.wait_send()
    for s in range(n_chunks):
        from_twin(0, data, s, s < wx_chunks).wait_send()
        relay(ynbr, 2, 1, data, s).wait_send()
        relay(znbr, 3, 2, data, s).wait_send()
        if s % 3 == 0:
            from_twin(3, diag, s, s < wx_chunks).wait_send()
        else:
            relay(ynbr, 3 + s % 3, 3, diag, s).wait_send()


def lstm(x, wx, wh, bias, h0, c0, tile=256):
    batch, steps, in_dim = x.shape
    rows = batch // 2
    hidden, units = wh.shape[1:]
    nb = 2 * (units // tile)
    n_chunks = (in_dim + hidden) // CH
    any_spec = pl.BlockSpec(memory_space=pl.ANY)

    def kernel(*refs):
        lstm_kernel(steps, rows, units, tile, in_dim, *refs)

    return pl.pallas_call(
        kernel,
        out_shape=(jax.ShapeDtypeStruct((steps, batch, units), BF16),
                   jax.ShapeDtypeStruct((batch, units), F32),
                   jax.ShapeDtypeStruct((batch, units), F32),
                   jax.ShapeDtypeStruct((steps, 4 * nb, rows, tile), F32)),
        in_specs=[any_spec] * 6,
        out_specs=(any_spec,) * 4,
        scratch_shapes=[
            pltpu.VMEM((2, 4, in_dim + hidden, units), BF16),
            pltpu.VMEM((SLOTS, 2, 2 * rows, nb * tile), BF16),
            pltpu.VMEM((nb, rows, tile), F32),
            pltpu.VMEM((nb, rows, tile), F32),
            pltpu.VMEM((nb, 4, rows, tile), F32),
            pltpu.VMEM((XSLOTS, 4 * nb, rows, tile), F32),
            pltpu.VMEM((2, 4, units), F32),
            pltpu.VMEM((2, rows, TX, in_dim), BF16),
            pltpu.VMEM((in_dim // 128, rows * TX, 128), F32),
            pltpu.VMEM((steps, rows, in_dim), BF16),
            pltpu.VMEM((2, TC, 2 * nb, rows, tile), F32),
            pltpu.SemaphoreType.DMA((5,)),
            pltpu.SemaphoreType.DMA((3, 1 + nb)),
            pltpu.SemaphoreType.DMA((4, n_chunks)),
            pltpu.SemaphoreType.DMA((6, n_chunks)),
            pltpu.SemaphoreType.DMA((2,)),
            pltpu.SemaphoreType.DMA((2,)),
            pltpu.SemaphoreType.DMA((XSLOTS,)),
            pltpu.SemaphoreType.DMA((SLOTS,)),
            pltpu.SemaphoreType.DMA((SLOTS,)),
            pltpu.SemaphoreType.DMA((SLOTS,)),
            pltpu.SemaphoreType.DMA((SLOTS,)),
            pltpu.SemaphoreType.DMA,
            pltpu.SemaphoreType.DMA((2, 2, nb)),
        ],
        compiler_params=pltpu.CompilerParams(
            collective_id=0, has_side_effects=True, vmem_limit_bytes=60 * 1024 * 1024),
        name="recurrent",
    )(x, wx, wh, bias, h0, c0)


def solution(mesh):
    def local_fn(x, w_in, w_rec, gate_bias, h_init, c_init):
        y, h_last, c_last, _ = lstm(x, w_in.swapaxes(0, 1), w_rec.swapaxes(0, 1), gate_bias, h_init, c_init)
        return y.swapaxes(0, 1), h_last, c_last

    return jax.shard_map(
        local_fn,
        mesh=mesh,
        in_specs=(P("data", None, None), P(None, None, "model"), P(None, None, "model"),
                  P(None, "model"), P("data", "model"), P("data", "model")),
        out_specs=(P("data", None, "model"), P("data", "model"), P("data", "model")),
        check_vma=False,
    )
```

```python
import jax
import jax.numpy as jnp
from jax import lax
from jax.experimental import pallas as pl
from jax.experimental.pallas import tpu as pltpu
from jax.sharding import PartitionSpec as P

MESH = pl.DeviceIdType.MESH
F32 = jnp.float32
BF16 = jnp.bfloat16
SLOTS = 4
XSLOTS = 3
TX = 16
TC = 8
LAG = 6
DELAY = 2
AHEAD = 5
CH = 128


def sigmoid(v):
    return 0.5 * jnp.tanh(0.5 * v) + 0.5


def lstm_kernel(steps, rows, units, tile, in_dim,
                x_ref, wx_ref, wh_ref, bias_ref, h0_ref, c0_ref,
                y_ref, hl_ref, cl_ref, xp_ref,
                w_ref, hbuf, c_ref, hf_ref, acc, xbuf, bias_v, xraw, xf, xt, xout,
                wsem, isem, rsem, ssem, insem, outsem,
                xsem, hsend, hrecv, ylocal, ysend, yrecv, fin):
    per = units // tile
    nb = 2 * per
    me = lax.axis_index("model")
    data = lax.axis_index("data")
    core = me % 2
    chip = me // 2
    sib = 2 * chip + (1 - core)
    twin = 2 * (1 - chip) + core
    sibtwin = 2 * (1 - chip) + (1 - core)
    ynbr = 2 * (data // 2) + (1 - data % 2)
    znbr = 2 * (1 - data // 2) + data % 2
    diag = 2 * (1 - data // 2) + (1 - data % 2)
    row0 = pl.multiple_of(chip * rows, rows)
    orow0 = pl.multiple_of((1 - chip) * rows, rows)

    hbuf[...] = jnp.zeros(hbuf.shape, BF16)
    barrier = pltpu.get_barrier_semaphore()
    for peer in ({"model": sib}, {"model": twin}, {"data": ynbr}, {"data": znbr}):
        pl.semaphore_signal(barrier, inc=1, device_id=peer, device_id_type=MESH)

    loads = [pltpu.make_async_copy(wx_ref, w_ref.at[0, :, pl.ds(0, in_dim), :], wsem.at[0])]
    for kb, blk in enumerate((me, twin, sib, sibtwin)):
        loads.append(pltpu.make_async_copy(
            wh_ref.at[:, pl.ds(pl.multiple_of(blk * units, units), units), :],
            w_ref.at[0, :, pl.ds(in_dim + kb * units, units), :],
            wsem.at[1 + kb]))
    for cp in loads:
        cp.start()

    def x_copy(n, slot):
        return pltpu.make_async_copy(
            x_ref.at[pl.ds(row0, rows), pl.ds(pl.multiple_of(n * TX, TX), TX)], xraw.at[slot], insem.at[slot])

    x_copy(0, 0).start()

    own_init = [pltpu.make_async_copy(bias_ref, bias_v.at[0], isem.at[0, 0])]
    for n in range(per):
        cols = pl.ds(n * tile, tile)
        own_init.append(pltpu.make_async_copy(h0_ref.at[pl.ds(row0, rows), cols], hf_ref.at[n], isem.at[0, 1 + n]))
        own_init.append(pltpu.make_async_copy(c0_ref.at[pl.ds(row0, rows), cols], c_ref.at[n], isem.at[0, 1 + per + n]))
    for cp in own_init:
        cp.start()

    pl.semaphore_wait(barrier, 4)

    n_chunks = (in_dim + 4 * units) // CH

    def landing(g, s):
        return w_ref.at[1, g, pl.ds(pl.multiple_of(s * CH, CH), CH), :]

    wx_chunks = in_dim // CH

    def from_twin(rel, g, s, of_wx):
        if of_wx:
            src = wx_ref.at[g, pl.ds(pl.multiple_of(s * CH, CH), CH), :]
        else:
            kb = (s - wx_chunks) * CH // units
            off = (s - wx_chunks) * CH % units
            blk = 2 * ((chip + 1 + kb) % 2) + (core + kb // 2) % 2
            src = wh_ref.at[g, pl.ds(pl.multiple_of(blk * units + off, CH), CH), :]
        return pltpu.make_async_remote_copy(
            src_ref=src, dst_ref=landing(g, s),
            send_sem=ssem.at[0 if rel == 0 else 1, s], recv_sem=rsem.at[rel, s],
            device_id={"model": twin}, device_id_type=MESH)

    def relay(peer, link, rel, g, s):
        return pltpu.make_async_remote_copy(
            src_ref=landing(g, s), dst_ref=landing(g, s),
            send_sem=ssem.at[link, s], recv_sem=rsem.at[rel, s],
            device_id={"data": peer}, device_id_type=MESH)

    other_init = [pltpu.make_async_remote_copy(
        src_ref=bias_ref, dst_ref=bias_v.at[1], send_sem=isem.at[1, 0], recv_sem=isem.at[2, 0],
        device_id={"model": twin}, device_id_type=MESH)]
    for n in range(per):
        cols = pl.ds(n * tile, tile)
        for src, dst, at in ((h0_ref, hf_ref, 1), (c0_ref, c_ref, 1 + per)):
            other_init.append(pltpu.make_async_remote_copy(
                src_ref=src.at[pl.ds(orow0, rows), cols], dst_ref=dst.at[per + n],
                send_sem=isem.at[1, at + n], recv_sem=isem.at[2, at + n],
                device_id={"model": twin}, device_id_type=MESH))
    for s in range(AHEAD):
        from_twin(0, data, s, True).start()
        if s % 3 == 0:
            from_twin(3, diag, s, True).start()
    for cp in other_init:
        cp.start()
    first_late = -(-wx_chunks // 3) * 3
    n_late = len(range(first_late, n_chunks, 3))

    def forward(s):
        relay(ynbr, 2, 0, data, s).wait_recv()
        relay(ynbr, 2, 1, data, s).start()
        relay(znbr, 3, 2, data, s).start()
        nxt = s + AHEAD

        @pl.when(nxt < wx_chunks)
        def _():
            from_twin(0, data, nxt, True).start()

            @pl.when(lax.rem(nxt, 3) == 0)
            def _():
                from_twin(3, diag, nxt, True).start()

        @pl.when(jnp.logical_and(nxt >= wx_chunks, nxt < n_chunks))
        def _():
            from_twin(0, data, nxt, False).start()

        @pl.when(s >= n_chunks - n_late)
        def _():
            from_twin(3, diag, first_late + 3 * (s - (n_chunks - n_late)), False).start()

    def forward_diag(s):
        relay(ynbr, 2, 1, data, s).wait_recv()
        relay(znbr, 3, 2, data, s).wait_recv()

        @pl.when(lax.rem(s, 3) == 1)
        def _():
            relay(ynbr, 4, 3, znbr, s).start()

        @pl.when(lax.rem(s, 3) == 2)
        def _():
            relay(znbr, 5, 3, ynbr, s).start()

    def stage(i):
        @pl.when(i < n_chunks)
        def _():
            forward(i)

        @pl.when(jnp.logical_and(i >= LAG, i < n_chunks + LAG))
        def _():
            forward_diag(i - LAG)

    def xout_copy(half, c, slot):
        return pltpu.make_async_copy(
            xout.at[slot], xp_ref.at[pl.ds(c * TC, TC), pl.ds(half * 4 * per, 4 * per)], outsem.at[slot])

    def project(it, carry):
        half = it // (steps // TC)
        c = lax.rem(it, steps // TC)
        slot = lax.rem(it, 2)

        late = it - steps // TC

        @pl.when(jnp.logical_and(it >= DELAY, late < 0))
        def _():
            stage(it - DELAY)

        @pl.when(jnp.logical_and(late >= 0, lax.rem(late, 3) < 2))
        def _():
            stage(steps // TC - DELAY + late // 3 * 2 + lax.rem(late, 3))

        @pl.when(it == steps // TC)
        def _():
            for s in range(in_dim // CH):
                relay(ynbr, 4, 3, diag, s).wait_recv()
            other_init[0].wait_recv()

        @pl.when(jnp.logical_and(slot == 0, half == 0))
        def _():
            n = it // 2
            xslot = lax.rem(n, 2)
            x_copy(n, xslot).wait()

            @pl.when(n + 1 < steps // TX)
            def _():
                x_copy(n + 1, 1 - xslot).start()

            for f in range(in_dim // 128):
                lanes = slice(f * 128, (f + 1) * 128)
                xf[f] = xraw[xslot, :, :, lanes].astype(F32).reshape(rows * TX, 128)
            for f in range(in_dim // 128):
                lanes = slice(f * 128, (f + 1) * 128)
                for tt in range(TX):
                    xt[n * TX + tt, :, lanes] = xf[f, pl.ds(tt, rows, stride=TX), :].astype(BF16)

        @pl.when(it >= 2)
        def _():
            xout_copy(half, c, slot).wait()

        xv = xt[pl.ds(c * TC, TC)].reshape(TC * rows, in_dim)
        for k in range(4):
            for nn in range(per):
                cols = slice(nn * tile, (nn + 1) * tile)
                g = jnp.dot(xv, w_ref[half, k, 0:in_dim, cols], preferred_element_type=F32)
                xout[slot, :, k * per + nn] = (g + bias_v[half, k:k + 1, cols]).reshape(TC, rows, tile)
        xout_copy(half, c, slot).start()
        return carry

    for cp in own_init + loads:
        cp.wait()
    n_proj = 2 * (steps // TC)
    lax.fori_loop(0, n_proj, project, 0)
    for slot in range(2):
        xout_copy(0, 0, slot).wait()

    def xcopy(t, slot):
        return pltpu.make_async_copy(xp_ref.at[t], xbuf.at[slot], xsem.at[slot])

    for t in range(XSLOTS):
        xcopy(t, t).start()

    def tail(i, carry):
        stage(i)
        return carry

    n_stages = steps // TC - DELAY + sum(i % 3 < 2 for i in range(steps // TC))
    lax.fori_loop(n_stages, max(n_stages, n_chunks + LAG), tail, 0)

    def hcopy(slot):
        return pltpu.make_async_remote_copy(
            src_ref=hbuf.at[slot, 0, pl.ds(0, rows)], dst_ref=hbuf.at[slot, 1, pl.ds(0, rows)],
            send_sem=hsend.at[slot], recv_sem=hrecv.at[slot],
            device_id={"model": sib}, device_id_type=MESH)

    def ylocal_copy(t, slot):
        return pltpu.make_async_copy(
            hbuf.at[slot, 0, pl.ds(0, rows), pl.ds(0, units)], y_ref.at[t, pl.ds(row0, rows)], ylocal.at[slot])

    def ytwin_copy(t, slot):
        return pltpu.make_async_remote_copy(
            src_ref=hbuf.at[slot, 0, pl.ds(0, rows), pl.ds(units, units)], dst_ref=y_ref.at[t, pl.ds(row0, rows)],
            send_sem=ysend.at[slot], recv_sem=yrecv,
            device_id={"model": twin}, device_id_type=MESH)

    def wait_y(slot):
        ylocal_copy(0, slot).wait()
        ytwin_copy(0, slot).wait_send()

    for cp in other_init[1:]:
        cp.wait_recv()
    for j in range(nb):
        hbuf[0, 0, 0:rows, j * tile:(j + 1) * tile] = hf_ref[j].astype(BF16)
    hcopy(0).start()
    deep = nb * tile
    cut = deep // 2

    def product(slot, side, j, k, lo, hi):
        half, nn = divmod(j, per)
        row = in_dim + side * deep
        w = w_ref[half, k, row + lo:row + hi, nn * tile:(nn + 1) * tile]
        return jnp.dot(hbuf[slot, side, :, lo:hi], w, preferred_element_type=F32)[:rows]

    def part_own(slot, xslot, stage):
        for j in range(nb):
            half, nn = divmod(j, per)
            for k in range(4):
                if j < nb // 2:
                    if stage == 0:
                        acc[j, k] = product(slot, 0, j, k, 0, cut) + xbuf[xslot, (half * 4 + k) * per + nn]
                    else:
                        acc[j, k] = product(slot, 0, j, k, cut, deep) + acc[j, k]
                elif stage == 1:
                    acc[j, k] = product(slot, 0, j, k, 0, deep) + xbuf[xslot, (half * 4 + k) * per + nn]

    def part_rest(slot, nslot, last):
        for j in range(nb):
            g = [product(slot, 1, j, k, 0, deep) + acc[j, k] for k in range(4)]
            c = sigmoid(g[1]) * c_ref[j] + sigmoid(g[0]) * jnp.tanh(g[3])
            c_ref[j] = c
            hv = sigmoid(g[2]) * jnp.tanh(c)
            hbuf[nslot, 0, 0:rows, j * tile:(j + 1) * tile] = hv.astype(BF16)
            if last:
                hf_ref[j] = hv

    own_chunks = (in_dim + deep) // CH
    for s in range(in_dim // CH, own_chunks):
        relay(ynbr, 4, 3, diag, s).wait_recv()
    xcopy(0, 0).wait()
    part_own(0, 0, 0)
    part_own(0, 0, 1)
    for s in range(own_chunks, n_chunks):
        relay(ynbr, 4, 3, diag, s).wait_recv()

    def step(t, carry):
        slot = lax.rem(t, SLOTS)
        nslot = lax.rem(t + 1, SLOTS)

        @pl.when(t >= SLOTS)
        def _():
            hcopy(nslot).wait_send()
            wait_y(nslot)

        @pl.when(t == SLOTS - 1)
        def _():
            hcopy(nslot).wait_send()

        @pl.when(t + XSLOTS < steps)
        def _():
            xcopy(t + XSLOTS, lax.rem(t, XSLOTS)).start()
        xslot = lax.rem(t + 1, XSLOTS)
        xcopy(0, xslot).wait()
        hcopy(slot).wait_recv()
        part_rest(slot, nslot, False)
        part_own(nslot, xslot, 0)
        hcopy(nslot).start()
        ylocal_copy(t, nslot).start()
        ytwin_copy(t, nslot).start()
        part_own(nslot, xslot, 1)
        return carry

    lax.fori_loop(0, steps - 1, step, 0)

    t = steps - 1
    slot, nslot = t % SLOTS, (t + 1) % SLOTS
    hcopy(nslot).wait_send()
    wait_y(nslot)
    hcopy(slot).wait_recv()
    part_rest(slot, nslot, True)
    ylocal_copy(t, nslot).start()
    ytwin_copy(t, nslot).start()

    ends = []
    for n, (src, dst) in enumerate(((hf_ref, hl_ref), (c_ref, cl_ref))):
        for j in range(nb):
            d = dst.at[pl.ds(row0, rows), pl.ds((j % per) * tile, tile)]
            if j < per:
                cp = pltpu.make_async_copy(src.at[j], d, fin.at[0, n, j])
            else:
                cp = pltpu.make_async_remote_copy(
                    src_ref=src.at[j], dst_ref=d,
                    send_sem=fin.at[0, n, j], recv_sem=fin.at[1, n, j],
                    device_id={"model": twin}, device_id_type=MESH)
            cp.start()
            ends.append(cp)
    for s in range(1, SLOTS):
        q = (nslot + s) % SLOTS
        hcopy(q).wait_send()
        wait_y(q)
    wait_y(nslot)
    theirs = y_ref.at[:, pl.ds(pl.multiple_of((1 - chip) * rows, rows), rows), :]
    pltpu.make_async_copy(theirs, theirs, yrecv).wait()
    for cp in ends:
        cp.wait()
    for cp in other_init:
        cp.wait_send()
    for s in range(n_chunks):
        from_twin(0, data, s, s < wx_chunks).wait_send()
        relay(ynbr, 2, 1, data, s).wait_send()
        relay(znbr, 3, 2, data, s).wait_send()
        if s % 3 == 0:
            from_twin(3, diag, s, s < wx_chunks).wait_send()
        else:
            relay(ynbr, 3 + s % 3, 3, diag, s).wait_send()


def lstm(x, wx, wh, bias, h0, c0, tile=256):
    batch, steps, in_dim = x.shape
    rows = batch // 2
    hidden, units = wh.shape[1:]
    nb = 2 * (units // tile)
    n_chunks = (in_dim + hidden) // CH
    any_spec = pl.BlockSpec(memory_space=pl.ANY)

    def kernel(*refs):
        lstm_kernel(steps, rows, units, tile, in_dim, *refs)

    return pl.pallas_call(
        kernel,
        out_shape=(jax.ShapeDtypeStruct((steps, batch, units), BF16),
                   jax.ShapeDtypeStruct((batch, units), F32),
                   jax.ShapeDtypeStruct((batch, units), F32),
                   jax.ShapeDtypeStruct((steps, 4 * nb, rows, tile), F32)),
        in_specs=[any_spec] * 6,
        out_specs=(any_spec,) * 4,
        scratch_shapes=[
            pltpu.VMEM((2, 4, in_dim + hidden, units), BF16),
            pltpu.VMEM((SLOTS, 2, 2 * rows, nb * tile), BF16),
            pltpu.VMEM((nb, rows, tile), F32),
            pltpu.VMEM((nb, rows, tile), F32),
            pltpu.VMEM((nb, 4, rows, tile), F32),
            pltpu.VMEM((XSLOTS, 4 * nb, rows, tile), F32),
            pltpu.VMEM((2, 4, units), F32),
            pltpu.VMEM((2, rows, TX, in_dim), BF16),
            pltpu.VMEM((in_dim // 128, rows * TX, 128), F32),
            pltpu.VMEM((steps, rows, in_dim), BF16),
            pltpu.VMEM((2, TC, 2 * nb, rows, tile), F32),
            pltpu.SemaphoreType.DMA((5,)),
            pltpu.SemaphoreType.DMA((3, 1 + nb)),
            pltpu.SemaphoreType.DMA((4, n_chunks)),
            pltpu.SemaphoreType.DMA((6, n_chunks)),
            pltpu.SemaphoreType.DMA((2,)),
            pltpu.SemaphoreType.DMA((2,)),
            pltpu.SemaphoreType.DMA((XSLOTS,)),
            pltpu.SemaphoreType.DMA((SLOTS,)),
            pltpu.SemaphoreType.DMA((SLOTS,)),
            pltpu.SemaphoreType.DMA((SLOTS,)),
            pltpu.SemaphoreType.DMA((SLOTS,)),
            pltpu.SemaphoreType.DMA,
            pltpu.SemaphoreType.DMA((2, 2, nb)),
        ],
        compiler_params=pltpu.CompilerParams(
            collective_id=0, has_side_effects=True, vmem_limit_bytes=60 * 1024 * 1024),
        name="recurrent",
    )(x, wx, wh, bias, h0, c0)


def solution(mesh):
    def local_fn(x, w_in, w_rec, gate_bias, h_init, c_init):
        y, h_last, c_last, _ = lstm(x, w_in.swapaxes(0, 1), w_rec.swapaxes(0, 1), gate_bias, h_init, c_init)
        return y.swapaxes(0, 1), h_last, c_last

    return jax.shard_map(
        local_fn,
        mesh=mesh,
        in_specs=(P("data", None, None), P(None, None, "model"), P(None, None, "model"),
                  P(None, "model"), P("data", "model"), P("data", "model")),
        out_specs=(P("data", None, "model"), P("data", "model"), P("data", "model")),
        check_vma=False,
    )
```
